32 devices in a mesh: ep: 8 (over z, y), dp: 4 (over x, core).
Axes of the slice: x: 2, y: 2, z: 4, core: 2. Of those that a mesh axis runs over, the one named last changes fastest.
Arguments:
- tokens_first: bfloat16 [4096, 2048], P(('ep', 'dp')), may hold values from -6 to 6
- routes_first: int32 [4096, 1], P(('ep', 'dp')), may hold values from 0 to 7; in each aligned block of 128 rows (0 to 127, 128 to 255, ...) at most 32 rows name the same one
- gates_first: bfloat16 [4096, 1], P(('ep', 'dp')), may hold values from 0.099609375 to 0.5
- gate_up_weight: bfloat16 [8, 2048, 768], P('ep'), may hold values from -0.125 to 0.125
- down_weight: bfloat16 [8, 384, 2048], P('ep'), may hold values from -0.3125 to 0.3125
- saved_inputs: bfloat16 [8, 4, 256, 2048], P('ep', 'dp'), may hold values from -6 to 6
- upstream: bfloat16 [4096, 2048], P(('ep', 'dp')), may hold values from -0.3984375 to 0.3984375
- routes_second: int32 [4096, 1], P(('ep', 'dp')), may hold values from 0 to 7; in each aligned block of 128 rows (0 to 127, 128 to 255, ...) at most 32 rows name the same one
- gates_second: bfloat16 [4096, 1], P(('ep', 'dp')), may hold values from 0.099609375 to 0.5
Outputs:
- mixed_first: bfloat16 [4096, 2048], P(('ep', 'dp'))
- gate_grads: float32 [4096, 1], P(('ep', 'dp'))
- gate_up_grad: bfloat16 [8, 2048, 768], P('ep', 'dp')
- down_grad: bfloat16 [8, 384, 2048], P('ep', None, 'dp')
The draws below stay inside these ranges and needn't reach their ends.
Inputs may be any that keep to these rules, and one draw needn't show every extreme that they name: `routes_first`: each row names 1 different experts; in the rows of one device no expert is named more than 32 times, a bound that some block reaches. `routes_second`: each row names 1 different experts; in the rows of one device no expert is named more than 32 times, a bound that some block reaches.
All inputs are finite; a program needn't handle non-finite values.
Results may differ from the reference program's by a relative error of at most 0.014.
Values may be sent and summed in bfloat16 or wider, within the bound.
A program may use at most 64 MiB of HBM per device.

```python
import math
import jax
import jax.numpy as jnp
import numpy as np
from jax import lax

D = 2048
HID = 384
TOP = 1
TOK_DEV = 128
EXPERTS = 8
CAP = 32
TOKENS = 4096
N_EP = 8
N_DP = 4


def strengthened(values, own_key, source, target, parts, factor):
    owner, partner = [(jnp.arange(values.shape[dim]) // (values.shape[dim] // parts)).reshape([-1 if axis == dim else 1 for axis in range(values.ndim)]) for dim in (source, target)]
    chosen = jax.random.permutation(own_key, parts)[partner]
    strong = (owner == chosen) | (owner == (partner + parts // 2) % parts)
    return jnp.where(strong, factor * values, values)


def steps_of(own_key, dims, pieces, least, top_value):
    def one(dim, parts):
        draws = jax.random.uniform(jax.random.fold_in(jax.random.fold_in(own_key, 6), dim), (parts,), jnp.float32, least / len(pieces), top_value / len(pieces))
        return jnp.repeat(jnp.exp(draws), dims[dim] // parts).reshape((-1,) + (1,) * (len(dims) - dim - 1))

    level = one(*pieces[0])
    for cut in pieces[1:]:
        level = level * one(*cut)
    return level


def routed_block(rng, own, number, rows, number_of, top, bound, skew):
    order = jax.random.permutation(rng, number_of)
    packed, ordinary = load_shares(number_of, rows * top, bound, skew, True), load_shares(number_of, rows * top, bound, skew, False)
    places = jnp.arange(number_of)

    def named(sizes, offset_by):
        used = int((sizes > 0).sum())
        fixed = max(1, used // 4)
        shifted = fixed + (places - fixed + offset_by * (used - fixed)) % max(1, number_of - fixed)
        return jnp.zeros((number_of,), jnp.int32).at[order[jnp.where(places < fixed, places, shifted)]].set(jnp.asarray(sizes, jnp.int32))

    sizes = jnp.where(number % 4 == 0, named(packed, number // 4), named(ordinary, number - number // 4 - 1))
    mixed = jax.random.permutation(jax.random.fold_in(own, 3), number_of)
    source_of, sink = mixed[0:number_of // 2 * 2:2], mixed[1:number_of // 2 * 2:2]
    margin = jnp.minimum(sizes[source_of] - 1, bound - sizes[sink]) // 2
    margin = jnp.where((source_of == order[0]) | (sink == order[0]) | (sizes[sink] == 0), 0, jnp.maximum(margin, 0))
    shifted = jax.random.randint(jax.random.fold_in(own, 4), (number_of // 2,), 0, 1 << 20) % (margin + 1)
    sizes = sizes.at[source_of].add(-shifted).at[sink].add(shifted)
    members = jnp.searchsorted(jnp.cumsum(sizes), jnp.arange(rows * top), side="right").astype(jnp.int32)
    grid = members.reshape(top, rows).T
    grid = grid[jax.random.permutation(jax.random.fold_in(own, 1), rows)]
    offset_by = jax.random.randint(jax.random.fold_in(own, 2), (rows, 1), 0, top)
    return jnp.take_along_axis(grid, (jnp.arange(top)[None, :] + offset_by) % top, axis=1)


def load_shares(count, total, reach, slope, full):
    weights = [(1 << 20) // math.isqrt(grade ** slope) + 1 for grade in range(1, count + 1)]
    largest = reach if full else min(reach, max(-(-total // count), total * weights[0] // sum(weights)))
    least = 1 if total - largest >= count - 1 else 0
    holding, rest = [largest] + [least] * (count - 1), total - largest - least * (count - 1)
    while rest > 0:
        free = [i for i in range(1, count) if holding[i] < largest] or [i for i in range(1, count) if holding[i] < reach]
        whole, remaining = sum([weights[i] for i in free]), rest
        for i in free:
            addition = min(reach - holding[i], max(1, remaining * weights[i] // whole), rest)
            holding[i] = holding[i] + addition
            rest = rest - addition
    return np.array(holding)


def normal_values(own_key, extent, deviation, reach, split=(), kind=jnp.bfloat16):
    values = jax.random.normal(own_key, extent, jnp.float32) * deviation
    if len(split) > 0:
        values = steps_of(own_key, extent, split, -0.22, 0.18) * values
    return jnp.clip(values, min=-reach, max=reach).astype(kind)


def heavy_noise(stream_key, dims, scale, reach, cuts, heavy, kind=jnp.bfloat16):
    values = scale * jax.random.normal(stream_key, dims, jnp.float32)
    if cuts:
        values = values * steps_of(stream_key, dims, cuts, -0.22, 0.18)
    return jnp.clip(strengthened(values, jax.random.fold_in(stream_key, 3), *heavy), -reach, reach).astype(kind)


def setup_inputs(seed: int = 0) -> dict:
    key_list = jax.random.split(jax.random.key(seed), 10)
    tokens_first = normal_values(key_list[0], (TOKENS, D), 1.0, 6.0, ((0, 32),))
    routes_first_keys = jax.random.split(jax.random.fold_in(key_list[1], 1), TOKENS // TOK_DEV)
    routes_first_turns = jax.random.permutation(jax.random.fold_in(key_list[1], 3), TOKENS // TOK_DEV)
    routes_first = jax.vmap(lambda own, number: routed_block(jax.random.fold_in(key_list[1], 2), own, number, TOK_DEV, EXPERTS, TOP, CAP, 2))(routes_first_keys, routes_first_turns).reshape((TOKENS, TOP))
    gates_first = jnp.clip(0.099609375 + 0.40039062 * jax.random.uniform(key_list[2], (TOKENS, TOP), jnp.float32) ** steps_of(key_list[2], (TOKENS, TOP), ((0, 32),), -0.2, 0.2), 0.099609375, 0.5).astype(jnp.bfloat16)
    gate_up_weight = normal_values(key_list[3], (EXPERTS, D, 2 * HID), D ** -0.5, 0.125, ((0, 8),))
    down_weight = normal_values(key_list[4], (EXPERTS, HID, D), HID ** -0.5, 0.3125, ((0, 8),))
    saved_inputs = heavy_noise(key_list[5], (EXPERTS, N_DP, N_EP * CAP, D), 1.0, 6.0, ((0, 8), (1, 4)), (1, 3, 4, 2.0))
    upstream = normal_values(key_list[6], (TOKENS, D), 0.05, 0.3984375, ((0, 32),))
    routes_second_keys = jax.random.split(jax.random.fold_in(key_list[7], 1), TOKENS // TOK_DEV)
    routes_second_turns = jax.random.permutation(jax.random.fold_in(key_list[7], 3), TOKENS // TOK_DEV)
    routes_second = jax.vmap(lambda own, number: routed_block(jax.random.fold_in(key_list[7], 2), own, number, TOK_DEV, EXPERTS, TOP, CAP, 2))(routes_second_keys, routes_second_turns).reshape((TOKENS, TOP))
    gates_second = jnp.clip(0.099609375 + 0.40039062 * jax.random.uniform(key_list[8], (TOKENS, TOP), jnp.float32) ** steps_of(key_list[8], (TOKENS, TOP), ((0, 32),), -0.2, 0.2), 0.099609375, 0.5).astype(jnp.bfloat16)
    return {"tokens_first": tokens_first, "routes_first": routes_first, "gates_first": gates_first, "gate_up_weight": gate_up_weight, "down_weight": down_weight, "saved_inputs": saved_inputs, "upstream": upstream, "routes_second": routes_second, "gates_second": gates_second}


def slot_index(routing):
    expert_ids = jnp.arange(EXPERTS, dtype=jnp.int32)
    onehot = (routing[:, :, None] == expert_ids).astype(jnp.int32)
    counts = jnp.sum(onehot, axis=1)
    before = jnp.cumsum(counts, axis=0) - counts
    return jnp.sum(onehot * before[:, None, :], axis=2).astype(jnp.int32)


def reference(tokens_first, routes_first, gates_first, gate_up_weight, down_weight, saved_inputs, upstream, routes_second, gates_second):
    devices = N_EP * N_DP
    highest = lax.Precision.HIGHEST
    first_float = tokens_first.reshape(devices, TOK_DEV, D).astype(jnp.float32)
    first_routes = routes_first.reshape(devices, TOK_DEV, TOP)
    first_gates = gates_first.reshape(devices, TOK_DEV, TOP).astype(jnp.float32)
    first_slots = jax.vmap(slot_index)(first_routes)
    upstream_float = upstream.reshape(devices, TOK_DEV, D).astype(jnp.float32)
    second_routes = routes_second.reshape(devices, TOK_DEV, TOP)
    second_gates = gates_second.reshape(devices, TOK_DEV, TOP).astype(jnp.float32)
    second_slots = jax.vmap(slot_index)(second_routes)
    slot_ids = jnp.arange(CAP, dtype=jnp.int32)

    def hits(routing, slots, expert_id):
        return ((routing == expert_id)[..., None] & (slots[..., None] == slot_ids)).astype(jnp.float32)

    def regroup(values):
        shaped = values.reshape((N_EP, N_DP, CAP) + values.shape[2:])
        return jnp.swapaxes(shaped, 0, 1).reshape((N_DP * N_EP * CAP,) + values.shape[2:])

    def per_expert(carry, expert_id):
        mixed_sum, gate_sum = carry
        weight_gu = gate_up_weight[expert_id]
        weight_down = down_weight[expert_id]
        hit_first = hits(first_routes, first_slots, expert_id)
        slot_rows = jnp.einsum("ntc,ntd->ncd", jnp.sum(hit_first, axis=2), first_float, precision=highest).astype(jnp.bfloat16)
        projected = jnp.dot(slot_rows.reshape(-1, D), weight_gu, preferred_element_type=jnp.float32)
        activated = (jax.nn.silu(projected[:, :HID]) * projected[:, HID:]).astype(jnp.bfloat16)
        expert_out = jnp.dot(activated, weight_down, preferred_element_type=jnp.float32).astype(jnp.bfloat16)
        expert_out = expert_out.reshape(devices, CAP, D).astype(jnp.float32)
        token_weight = jnp.einsum("ntkc,ntk->ntc", hit_first, first_gates, precision=highest)
        mixed_sum = mixed_sum + jnp.einsum("ntc,ncd->ntd", token_weight, expert_out, precision=highest)

        hit_second = hits(second_routes, second_slots, expert_id)
        grad_slots = jnp.einsum("ntc,ntd->ncd", jnp.sum(hit_second, axis=2), upstream_float, precision=highest).astype(jnp.bfloat16)
        slot_gates = jnp.einsum("ntkc,ntk->nc", hit_second, second_gates, precision=highest)
        grad_group = regroup(grad_slots)
        gate_group = regroup(slot_gates).reshape(-1, 1)
        saved_rows = saved_inputs[expert_id].reshape(-1, D)
        projected_b = jnp.dot(saved_rows, weight_gu, preferred_element_type=jnp.float32)
        gate_part = projected_b[:, :HID]
        up_part = projected_b[:, HID:]
        squash = jax.nn.sigmoid(gate_part)
        swish = jax.nn.silu(gate_part)
        activated_b = (swish * up_part).astype(jnp.bfloat16)
        grad_hidden = lax.dot_general(grad_group, weight_down, (((1,), (1,)), ((), ())), preferred_element_type=jnp.float32)
        slot_value = jnp.sum(grad_hidden * activated_b.astype(jnp.float32), axis=1)
        slot_back = jnp.swapaxes(slot_value.reshape(N_DP, N_EP, CAP), 0, 1).reshape(devices, CAP)
        gate_sum = gate_sum + jnp.einsum("ntkc,nc->ntk", hit_second, slot_back, precision=highest)
        grad_scaled = gate_group * grad_hidden
        grad_gate = grad_scaled * up_part * squash * (1.0 + gate_part * (1.0 - squash))
        grad_up = grad_scaled * swish
        grad_both = jnp.concatenate([grad_gate, grad_up], axis=1).astype(jnp.bfloat16)
        grad_rows = (gate_group * grad_group.astype(jnp.float32)).astype(jnp.bfloat16)
        group_inputs = saved_rows.reshape(N_DP, -1, D).astype(jnp.float32)
        term_gu = jnp.einsum("nrd,nrj->ndj", group_inputs, grad_both.reshape(N_DP, -1, 2 * HID).astype(jnp.float32), precision=highest).astype(jnp.bfloat16)
        grad_gu = jnp.sum(term_gu.astype(jnp.float32), axis=0).astype(jnp.bfloat16)
        term_down = jnp.einsum("nrh,nrd->nhd", activated_b.reshape(N_DP, -1, HID).astype(jnp.float32), grad_rows.reshape(N_DP, -1, D).astype(jnp.float32), precision=highest).astype(jnp.bfloat16)
        grad_dn = jnp.sum(term_down.astype(jnp.float32), axis=0).astype(jnp.bfloat16)
        return (mixed_sum, gate_sum), (grad_gu, grad_dn)

    start = (jnp.zeros((devices, TOK_DEV, D), jnp.float32), jnp.zeros((devices, TOK_DEV, TOP), jnp.float32))
    (mixed_sum, gate_sum), (gu_all, down_all) = lax.scan(per_expert, start, jnp.arange(EXPERTS, dtype=jnp.int32))
    return (mixed_sum.reshape(TOKENS, D).astype(jnp.bfloat16), gate_sum.reshape(TOKENS, TOP), gu_all, down_all)
```

```python
import functools

import jax
import jax.numpy as jnp
from jax import lax
from jax.experimental import pallas as pl
from jax.experimental.pallas import tpu as pltpu
from jax.sharding import PartitionSpec as P


def slot_places(routing, experts, capacity):
    expert_ids = jnp.arange(experts, dtype=jnp.int32)
    onehot = (routing[:, :, None] == expert_ids).astype(jnp.int32)
    counts = jnp.sum(onehot, axis=1)
    before = jnp.cumsum(counts, axis=0) - counts
    slots = jnp.sum(onehot * before[:, None, :], axis=2)
    return routing * capacity + slots


def local_plain(
    tokens_first,
    routes_first,
    gates_first,
    gate_up_weight,
    down_weight,
    saved_inputs,
    upstream,
    routes_second,
    gates_second,
):
    experts = lax.axis_size("ep")
    capacity = saved_inputs.shape[2] // experts
    places = experts * capacity
    model_width = tokens_first.shape[1]
    weight_gu = gate_up_weight[0]
    weight_down = down_weight[0]
    hidden_size = weight_down.shape[0]

    def expand(places_of):
        lookup = (places_of[:, :, None] == jnp.arange(places, dtype=jnp.int32)).astype(jnp.bfloat16)
        return (lookup, jnp.sum(lookup, axis=1))

    def dispatch(select, values):
        moved = lax.dot_general(
            select, values, (((0,), (0,)), ((), ())), preferred_element_type=jnp.float32
        )
        return moved.astype(jnp.bfloat16).reshape(experts, capacity, model_width)

    def project(inputs):
        return jnp.dot(inputs, weight_gu, preferred_element_type=jnp.float32)

    first_places = slot_places(routes_first, experts, capacity)
    first_lookup, first_select = expand(first_places)
    send_first = dispatch(first_select, tokens_first)
    second_places = slot_places(routes_second, experts, capacity)
    second_lookup, second_select = expand(second_places)
    send_grad = dispatch(second_select, upstream)
    send_gates = jnp.einsum(
        "tkp,tk->p",
        second_lookup.astype(jnp.float32),
        gates_second.astype(jnp.float32),
        precision=lax.Precision.HIGHEST,
    )
    send_gates = send_gates.astype(jnp.bfloat16).reshape(experts, capacity)
    received = lax.all_to_all(send_first, "ep", split_axis=0, concat_axis=0, tiled=True)
    sources = received.shape[0]
    items = received.shape[1]
    projected = project(received.reshape(sources * items, model_width))
    activated = (jax.nn.silu(projected[:, :hidden_size]) * projected[:, hidden_size:]).astype(
        jnp.bfloat16
    )
    outputs = jnp.dot(activated, weight_down, preferred_element_type=jnp.float32).astype(
        jnp.bfloat16
    )
    returned = lax.all_to_all(
        outputs.reshape(sources, items, model_width), "ep", split_axis=0, concat_axis=0, tiled=True
    )
    arrived_grad, arrived_gates = (
        lax.all_to_all(send_grad, "ep", split_axis=0, concat_axis=0, tiled=True),
        lax.all_to_all(send_gates, "ep", split_axis=0, concat_axis=0, tiled=True),
    )
    picked = returned.reshape(places, model_width)[first_places]
    mixed_first = jnp.sum(
        gates_first.astype(jnp.float32)[:, :, None] * picked.astype(jnp.float32), axis=1
    ).astype(jnp.bfloat16)
    saved_rows = saved_inputs[0, 0]
    projected_b = project(saved_rows)
    gate_part = projected_b[:, :hidden_size]
    up_part = projected_b[:, hidden_size:]
    squash = jax.nn.sigmoid(gate_part)
    swish = jax.nn.silu(gate_part)
    activated_b = (swish * up_part).astype(jnp.bfloat16)
    incoming = arrived_grad.reshape(places, model_width)
    gate_column = arrived_gates.reshape(places, 1).astype(jnp.float32)
    grad_hidden = lax.dot_general(
        incoming, weight_down, (((1,), (1,)), ((), ())), preferred_element_type=jnp.float32
    )
    slot_value = jnp.sum(grad_hidden * activated_b.astype(jnp.float32), axis=1)
    returned_value = lax.all_to_all(
        slot_value.reshape(experts, capacity), "ep", split_axis=0, concat_axis=0, tiled=True
    )
    gate_grads = returned_value.reshape(places)[second_places]
    grad_scaled = gate_column * grad_hidden
    grad_gate = grad_scaled * up_part * squash * (1.0 + gate_part * (1.0 - squash))
    grad_up = grad_scaled * swish
    grad_both = jnp.concatenate([grad_gate, grad_up], axis=1).astype(jnp.bfloat16)
    grad_rows = (gate_column * incoming.astype(jnp.float32)).astype(jnp.bfloat16)
    down_term = lax.dot_general(
        activated_b, grad_rows, (((0,), (0,)), ((), ())), preferred_element_type=jnp.float32
    )
    gate_up_term = lax.dot_general(
        saved_rows, grad_both, (((0,), (0,)), ((), ())), preferred_element_type=jnp.float32
    )
    gate_up_grad, down_grad = (
        lax.psum_scatter(
            gate_up_term[None].astype(jnp.bfloat16), "dp", scatter_dimension=1, tiled=True
        ).astype(jnp.float32),
        lax.psum_scatter(
            down_term[None].astype(jnp.bfloat16), "dp", scatter_dimension=2, tiled=True
        ).astype(jnp.float32),
    )
    return (
        mixed_first,
        gate_grads,
        gate_up_grad.astype(jnp.bfloat16),
        down_grad.astype(jnp.bfloat16),
    )


MESH = pl.DeviceIdType.MESH
F32 = jnp.float32
BF16 = jnp.bfloat16


def flipped(index, offset):
    result, bit = index, 1
    while bit <= offset:
        if offset & bit:
            result = result + bit * (1 - 2 * ((index // bit) % 2))
        bit *= 2
    return result


def kernel(
    n_ep,
    n_dp,
    cap,
    routes_1_hbm,
    gates_1_hbm,
    routes_2_hbm,
    gates_2_hbm,
    tokens_hbm,
    upstream_hbm,
    gu_hbm,
    down_hbm,
    saved_hbm,
    rets,
    lookup,
    ggrad_ref,
    gu_out,
    dn_out,
    routes_1,
    gates_1,
    routes_2,
    gates_2,
    tokens,
    upstream,
    gu,
    down,
    saved,
    send_1,
    send_2,
    recv_1,
    recv_2,
    outs,
    proj,
    act_b,
    both,
    val_send,
    val_recv,
    term_gu,
    term_dn,
    pair_gu,
    pair_dn,
    sum_gu,
    sum_dn,
    far_gu,
    far_dn,
    in_sem,
    d2_send,
    d2_recv,
    d1_send,
    d1_recv,
    r1_send,
    r1_recv,
    v_send,
    v_recv,
    p_send,
    p_recv,
    f_send,
    f_recv,
):
    me = lax.axis_index("ep")
    me_dp = lax.axis_index("dp")
    parity, chip = me_dp % 2, me_dp // 2
    half = n_dp // 2
    mate = me_dp + 1 - 2 * parity
    count, width = tokens.shape
    hidden = down.shape[0]
    places = n_ep * cap
    middle = n_ep // 2
    near = list(range(middle - 1, 0, -1))
    cross = list(range(middle, n_ep))
    order = near + cross

    barrier = pltpu.get_barrier_semaphore()
    for d in range(n_ep - 1, 0, -1):
        pl.semaphore_signal(
            barrier, inc=1, device_id=(flipped(me, d), me_dp), device_id_type=MESH
        )
    pl.semaphore_signal(barrier, inc=1, device_id=(me, mate), device_id_type=MESH)
    for t in range(1, half):
        pl.semaphore_signal(
            barrier,
            inc=1,
            device_id=(me, 2 * ((chip + t) % half) + parity),
            device_id_type=MESH,
        )

    loads = [
        pltpu.make_async_copy(source, target, in_sem.at[k])
        for k, (source, target) in enumerate(
            (
                (routes_2_hbm, routes_2),
                (gates_2_hbm, gates_2),
                (upstream_hbm, upstream),
                (routes_1_hbm, routes_1),
                (gates_1_hbm, gates_1),
                (tokens_hbm, tokens),
                (saved_hbm, saved),
                (gu_hbm, gu),
                (down_hbm, down),
            )
        )
    ]
    for copy in loads[:3]:
        copy.start()

    def remote(source, target, sends, recvs, to):
        return pltpu.make_async_remote_copy(
            src_ref=source,
            dst_ref=target,
            send_sem=sends,
            recv_sem=recvs,
            device_id=to,
            device_id_type=MESH,
        )

    def placed(routes_ref):
        routes = routes_ref[...]
        rank = lax.broadcasted_iota(jnp.int32, (max(n_ep, 16), count), 0)
        named = jnp.where(rank == routes, 1.0, 0.0)
        earlier = jnp.where(
            lax.broadcasted_iota(jnp.int32, (count, count), 0)
            < lax.broadcasted_iota(jnp.int32, (count, count), 1),
            1.0,
            0.0,
        ).astype(BF16)
        before = jnp.dot(named.astype(BF16), earlier, preferred_element_type=F32)
        slots = jnp.sum(named * before, axis=0, keepdims=True).astype(jnp.int32)
        offset = jnp.bitwise_xor(routes, me)
        return offset, slots

    def column(row):
        return jnp.broadcast_to(row.astype(F32), (count, count)).T

    def spread(select, values, target, low, high):
        target[low:high] = (
            jnp.dot(select[low * cap : high * cap], values[...], preferred_element_type=F32)
            .astype(BF16)
            .reshape(high - low, cap, width)
        )

    slot_ids = lax.broadcasted_iota(jnp.int32, (places, count), 0)

    def turned(d):
        if d == 1:
            return d, flipped(me, 1)
        base = flipped(me, d - d % 2)
        swap = parity + (d % 2) * (1 - 2 * parity)
        return d - d % 2 + swap, base + swap * (1 - 2 * (base % 2))

    def sent_2(d):
        d, to = turned(d)
        return remote(send_2.at[d], recv_2.at[me], d2_send.at[d], d2_recv.at[d], (to, me_dp))

    def sent_1(d):
        d, to = turned(d)
        return remote(send_1.at[d], recv_1.at[d], d1_send.at[d], d1_recv.at[d], (to, me_dp))

    def sent_r(d):
        d, to = turned(d)
        return remote(outs.at[d], rets.at[d], r1_send.at[d], r1_recv.at[d], (to, me_dp))

    move_2 = {d: sent_2(d) for d in order}
    move_1 = {d: sent_1(d) for d in order}
    move_r = {d: sent_r(d) for d in order}

    loads[0].wait()
    offset_2, slot_2 = placed(routes_2)
    place_2 = offset_2 * cap + slot_2
    loads[1].wait()
    gate_row_2 = gates_2[...].astype(F32)
    select_2 = jnp.where(slot_ids == place_2, gate_row_2, 0.0).astype(BF16)
    loads[2].wait()
    for copy in loads[3:]:
        copy.start()
    spread(select_2, upstream, send_2, 0, middle)
    pl.semaphore_wait(barrier, n_ep - 1 + half)
    for d in near:
        move_2[d].start()
    spread(select_2, upstream, send_2, middle, n_ep)
    for d in cross:
        move_2[d].start()
    recv_2[me] = send_2[0]

    loads[3].wait()
    loads[4].wait()
    offset_1, slot_1 = placed(routes_1)
    place_1 = offset_1 * cap + slot_1
    select_1 = jnp.where(slot_ids == place_1, 1.0, 0.0).astype(BF16)
    loads[5].wait()
    spread(select_1, tokens, send_1, 0, n_ep)
    recv_1[0] = send_1[0]

    for d in order:
        move_1[d].start()

    place_col = column(place_1)
    gate_col = column(gates_1[...])
    lane_col = lax.broadcasted_iota(jnp.int32, (count, 128), 1).astype(F32)
    for part in range(places // 128):
        lookup[:, part * 128 : (part + 1) * 128] = jnp.where(
            place_col[:, :128] == lane_col + float(128 * part), gate_col[:, :128], 0.0
        ).astype(BF16)

    loads[6].wait()
    loads[7].wait()
    proj[...] = jnp.dot(saved[...], gu[...], preferred_element_type=F32)
    gate = proj[:, :hidden]
    act_b[...] = (gate * jax.nn.sigmoid(gate) * proj[:, hidden:]).astype(BF16)
    loads[8].wait()

    for d in order:
        move_2[d].wait_recv()

    incoming = recv_2[...].reshape(places, width)
    scaled = lax.dot_general(
        incoming, down[...], (((1,), (1,)), ((), ())), preferred_element_type=F32
    )
    product = scaled * act_b[...].astype(F32)
    lanes = product[:, :128]
    for first in range(128, hidden, 128):
        lanes = lanes + product[:, first : first + 128]
    values = jnp.sum(lanes.T, axis=0, keepdims=True)
    val_send[...] = values
    val_recv[0] = values
    move_v = {}
    for d in order:
        move_v[d] = remote(
            val_send, val_recv.at[d], v_send.at[d], v_recv.at[d], (flipped(me, d), me_dp)
        )
        move_v[d].start()
    gate = proj[:, :hidden]
    squash = jax.nn.sigmoid(gate)
    both[:, :hidden] = (
        scaled * proj[:, hidden:] * squash * (1.0 + gate * (1.0 - squash))
    ).astype(BF16)
    both[:, hidden:] = (scaled * (gate * squash)).astype(BF16)

    rows_gu = width // n_dp
    activated_b = act_b[...]
    for j in range(n_dp):
        term_gu[j] = lax.dot_general(
            saved[:, j * rows_gu : (j + 1) * rows_gu],
            both[...],
            (((0,), (0,)), ((), ())),
            preferred_element_type=F32,
        ).astype(BF16)
        term_dn[j] = lax.dot_general(
            activated_b,
            incoming[:, j * rows_gu : (j + 1) * rows_gu],
            (((0,), (0,)), ((), ())),
            preferred_element_type=F32,
        ).astype(BF16)
    move_p = []
    for k in range(half):
        for kind, (term, pair) in enumerate(((term_gu, pair_gu), (term_dn, pair_dn))):
            copy = remote(
                term.at[2 * k + 1 - parity],
                pair.at[k],
                p_send.at[kind, k],
                p_recv.at[kind, k],
                (me, mate),
            )
            copy.start()
            move_p.append(copy)
    for copy in move_p:
        copy.wait_recv()
    move_f = []
    for t in range(1, half):
        k = (chip + t) % half
        for kind, (term, pair, joint, far) in enumerate(
            ((term_gu, pair_gu, sum_gu, far_gu), (term_dn, pair_dn, sum_dn, far_dn))
        ):
            joint[t - 1] = (
                term[2 * k + parity].astype(F32) + pair[k].astype(F32)
            ).astype(BF16)
            copy = remote(
                joint.at[t - 1],
                far.at[t - 1],
                f_send.at[kind, t - 1],
                f_recv.at[kind, t - 1],
                (me, 2 * k + parity),
            )
            copy.start()
            move_f.append(copy)

    groups = list(range(n_ep // 4 - 1, -1, -1)) + list(range(n_ep // 4, n_ep // 2))
    for g in groups:
        for d in (2 * g, 2 * g + 1):
            if d:
                move_1[d].wait_recv()
        rows = recv_1[2 * g : 2 * g + 2].reshape(2 * cap, width)
        projected = jnp.dot(rows, gu[...], preferred_element_type=F32)
        first_gate = projected[:, :hidden]
        activated = (first_gate * jax.nn.sigmoid(first_gate) * projected[:, hidden:]).astype(BF16)
        outs[2 * g : 2 * g + 2] = (
            jnp.dot(activated, down[...], preferred_element_type=F32)
            .astype(BF16)
            .reshape(2, cap, width)
        )
        for d in (2 * g, 2 * g + 1):
            if d:
                move_r[d].start()
            else:
                rets[0] = outs[0]

    for d in order:
        move_v[d].wait_recv()
    offset_col = column(offset_2)
    wanted = column(slot_2 + me * cap)
    lane_ids = lax.broadcasted_iota(jnp.int32, (count, 128), 1).astype(F32)
    picked = jnp.zeros((count, 128), F32)
    for part in range(places // 128):
        for d in range(n_ep):
            hit = (offset_col[:, :128] == float(d)) & (wanted[:, :128] == lane_ids + 128.0 * part)
            picked = picked + jnp.where(hit, val_recv[d, :, part * 128 : (part + 1) * 128], 0.0)
    ggrad_ref[...] = jnp.sum(picked.T, axis=0, keepdims=True) / gate_row_2

    for copy in move_f:
        copy.wait_recv()
    for term, pair, far, out in (
        (term_gu, pair_gu, far_gu, gu_out),
        (term_dn, pair_dn, far_dn, dn_out),
    ):
        result = term[me_dp].astype(F32) + pair[chip].astype(F32)
        for t in range(1, half):
            result = result + far[t - 1].astype(F32)
        out[...] = result.astype(BF16)

    for d in order:
        move_2[d].wait_send()
        move_1[d].wait_send()
        move_v[d].wait_send()
    for copy in move_p + move_f:
        copy.wait_send()
    for d in order:
        move_r[d].wait_recv()
    for d in order:
        move_r[d].wait_send()


def finish(
    rets, lookup, ggrad, gu_grad, dn_grad, mixed_hbm, ggrad_hbm, gu_hbm, dn_hbm, mixed, out_sem
):
    stores = [
        pltpu.make_async_copy(source, target, out_sem.at[k])
        for k, (source, target) in enumerate(
            ((gu_grad, gu_hbm), (dn_grad, dn_hbm), (ggrad, ggrad_hbm))
        )
    ]
    for copy in stores:
        copy.start()
    width = mixed.shape[1]
    slots = rets.shape[0] * rets.shape[1]
    step = width // 4
    for number in range(4):
        columns = slice(number * step, (number + 1) * step)
        mixed[:, columns] = jnp.dot(
            lookup[...], rets[:, :, columns].reshape(slots, step), preferred_element_type=F32
        ).astype(BF16)
        copy = pltpu.make_async_copy(
            mixed.at[:, columns], mixed_hbm.at[:, columns], out_sem.at[3 + number]
        )
        copy.start()
        stores.append(copy)
    for copy in stores:
        copy.wait()


def local(
    tokens_first,
    routes_first,
    gates_first,
    gate_up_weight,
    down_weight,
    saved_inputs,
    upstream,
    routes_second,
    gates_second,
):
    n_ep, n_dp = lax.axis_size("ep"), lax.axis_size("dp")
    cap = saved_inputs.shape[2] // n_ep
    count, top = routes_first.shape
    width = tokens_first.shape[1]
    hidden = down_weight.shape[1]
    places = n_ep * cap
    fits = (
        top == 1
        and cap % 16 == 0
        and 2 * cap <= 128
        and count == 128
        and places % 128 == 0
        and hidden % 128 == 0
        and n_ep >= 4
        and n_ep & (n_ep - 1) == 0
        and n_dp >= 4
        and n_dp % 2 == 0
        and (width // n_dp) % 128 == 0
    )
    if not fits:
        return local_plain(
            tokens_first,
            routes_first,
            gates_first,
            gate_up_weight,
            down_weight,
            saved_inputs,
            upstream,
            routes_second,
            gates_second,
        )
    half, part = n_dp // 2, width // n_dp
    slots = pltpu.VMEM((n_ep, cap, width), BF16)
    dma = pltpu.SemaphoreType.DMA
    vmem, anywhere = pl.BlockSpec(memory_space=pltpu.VMEM), pl.BlockSpec(memory_space=pl.ANY)
    reached = pl.pallas_call(
        functools.partial(kernel, n_ep, n_dp, cap),
        out_shape=(
            slots,
            pltpu.VMEM((count, places), BF16),
            pltpu.VMEM((1, count), F32),
            pltpu.VMEM((part, 2 * hidden), BF16),
            pltpu.VMEM((hidden, part), BF16),
        ),
        in_specs=[anywhere] * 9,
        out_specs=(vmem,) * 5,
        scratch_shapes=[
            pltpu.VMEM((1, count), jnp.int32),
            pltpu.VMEM((1, count), BF16),
            pltpu.VMEM((1, count), jnp.int32),
            pltpu.VMEM((1, count), BF16),
            pltpu.VMEM((count, width), BF16),
            pltpu.VMEM((count, width), BF16),
            pltpu.VMEM((width, 2 * hidden), BF16),
            pltpu.VMEM((hidden, width), BF16),
            pltpu.VMEM((places, width), BF16),
            slots,
            slots,
            slots,
            slots,
            slots,
            pltpu.VMEM((places, 2 * hidden), F32),
            pltpu.VMEM((places, hidden), BF16),
            pltpu.VMEM((places, 2 * hidden), BF16),
            pltpu.VMEM((1, places), F32),
            pltpu.VMEM((n_ep, 1, places), F32),
            pltpu.VMEM((n_dp, part, 2 * hidden), BF16),
            pltpu.VMEM((n_dp, hidden, part), BF16),
            pltpu.VMEM((half, part, 2 * hidden), BF16),
            pltpu.VMEM((half, hidden, part), BF16),
            pltpu.VMEM((half - 1, part, 2 * hidden), BF16),
            pltpu.VMEM((half - 1, hidden, part), BF16),
            pltpu.VMEM((half - 1, part, 2 * hidden), BF16),
            pltpu.VMEM((half - 1, hidden, part), BF16),
            dma((9,)),
        ]
        + [dma((n_ep,))] * 8
        + [dma((2, half))] * 2
        + [dma((2, half - 1))] * 2,
        compiler_params=pltpu.CompilerParams(
            collective_id=0, has_side_effects=True, vmem_limit_bytes=44 * 1024 * 1024
        ),
    )(
        *(
            pltpu.with_memory_space_constraint(value, pltpu.HBM)
            for value in (
                routes_first.reshape(1, count),
                gates_first.reshape(1, count),
                routes_second.reshape(1, count),
                gates_second.reshape(1, count),
                tokens_first,
                upstream,
                gate_up_weight[0],
                down_weight[0],
                saved_inputs[0, 0],
            )
        )
    )
    mixed, gate_grads, gu_grad, dn_grad = pl.pallas_call(
        finish,
        out_shape=(
            jax.ShapeDtypeStruct((count, width), BF16),
            jax.ShapeDtypeStruct((1, count), F32),
            jax.ShapeDtypeStruct((part, 2 * hidden), BF16),
            jax.ShapeDtypeStruct((hidden, part), BF16),
        ),
        in_specs=[vmem] * 5,
        out_specs=(anywhere,) * 4,
        scratch_shapes=[pltpu.VMEM((count, width), BF16), dma((7,))],
        name="finish",
    )(*(pltpu.with_memory_space_constraint(value, pltpu.VMEM) for value in reached))
    return mixed, gate_grads.reshape(count, 1), gu_grad[None], dn_grad[None]


def solution(mesh):
    return jax.shard_map(
        local,
        mesh=mesh,
        in_specs=(
            P(("ep", "dp"), None),
            P(("ep", "dp"), None),
            P(("ep", "dp"), None),
            P("ep", None, None),
            P("ep", None, None),
            P("ep", "dp", None, None),
            P(("ep", "dp"), None),
            P(("ep", "dp"), None),
            P(("ep", "dp"), None),
        ),
        out_specs=(
            P(("ep", "dp"), None),
            P(("ep", "dp"), None),
            P("ep", "dp", None),
            P("ep", None, "dp"),
        ),
        check_vma=False,
    )
```

```python
import functools

import jax
import jax.numpy as jnp
from jax import lax
from jax.experimental import pallas as pl
from jax.experimental.pallas import tpu as pltpu
from jax.sharding import PartitionSpec as P


def slot_places(routing, experts, capacity):
    expert_ids = jnp.arange(experts, dtype=jnp.int32)
    onehot = (routing[:, :, None] == expert_ids).astype(jnp.int32)
    counts = jnp.sum(onehot, axis=1)
    before = jnp.cumsum(counts, axis=0) - counts
    slots = jnp.sum(onehot * before[:, None, :], axis=2)
    return routing * capacity + slots


def local_plain(
    tokens_first,
    routes_first,
    gates_first,
    gate_up_weight,
    down_weight,
    saved_inputs,
    upstream,
    routes_second,
    gates_second,
):
    experts = lax.axis_size("ep")
    capacity = saved_inputs.shape[2] // experts
    places = experts * capacity
    model_width = tokens_first.shape[1]
    weight_gu = gate_up_weight[0]
    weight_down = down_weight[0]
    hidden_size = weight_down.shape[0]

    def expand(places_of):
        lookup = (places_of[:, :, None] == jnp.arange(places, dtype=jnp.int32)).astype(jnp.bfloat16)
        return (lookup, jnp.sum(lookup, axis=1))

    def dispatch(select, values):
        moved = lax.dot_general(
            select, values, (((0,), (0,)), ((), ())), preferred_element_type=jnp.float32
        )
        return moved.astype(jnp.bfloat16).reshape(experts, capacity, model_width)

    def project(inputs):
        return jnp.dot(inputs, weight_gu, preferred_element_type=jnp.float32)

    first_places = slot_places(routes_first, experts, capacity)
    first_lookup, first_select = expand(first_places)
    send_first = dispatch(first_select, tokens_first)
    second_places = slot_places(routes_second, experts, capacity)
    second_lookup, second_select = expand(second_places)
    send_grad = dispatch(second_select, upstream)
    send_gates = jnp.einsum(
        "tkp,tk->p",
        second_lookup.astype(jnp.float32),
        gates_second.astype(jnp.float32),
        precision=lax.Precision.HIGHEST,
    )
    send_gates = send_gates.astype(jnp.bfloat16).reshape(experts, capacity)
    received = lax.all_to_all(send_first, "ep", split_axis=0, concat_axis=0, tiled=True)
    sources = received.shape[0]
    items = received.shape[1]
    projected = project(received.reshape(sources * items, model_width))
    activated = (jax.nn.silu(projected[:, :hidden_size]) * projected[:, hidden_size:]).astype(
        jnp.bfloat16
    )
    outputs = jnp.dot(activated, weight_down, preferred_element_type=jnp.float32).astype(
        jnp.bfloat16
    )
    returned = lax.all_to_all(
        outputs.reshape(sources, items, model_width), "ep", split_axis=0, concat_axis=0, tiled=True
    )
    arrived_grad, arrived_gates = (
        lax.all_to_all(send_grad, "ep", split_axis=0, concat_axis=0, tiled=True),
        lax.all_to_all(send_gates, "ep", split_axis=0, concat_axis=0, tiled=True),
    )
    picked = returned.reshape(places, model_width)[first_places]
    mixed_first = jnp.sum(
        gates_first.astype(jnp.float32)[:, :, None] * picked.astype(jnp.float32), axis=1
    ).astype(jnp.bfloat16)
    saved_rows = saved_inputs[0, 0]
    projected_b = project(saved_rows)
    gate_part = projected_b[:, :hidden_size]
    up_part = projected_b[:, hidden_size:]
    squash = jax.nn.sigmoid(gate_part)
    swish = jax.nn.silu(gate_part)
    activated_b = (swish * up_part).astype(jnp.bfloat16)
    incoming = arrived_grad.reshape(places, model_width)
    gate_column = arrived_gates.reshape(places, 1).astype(jnp.float32)
    grad_hidden = lax.dot_general(
        incoming, weight_down, (((1,), (1,)), ((), ())), preferred_element_type=jnp.float32
    )
    slot_value = jnp.sum(grad_hidden * activated_b.astype(jnp.float32), axis=1)
    returned_value = lax.all_to_all(
        slot_value.reshape(experts, capacity), "ep", split_axis=0, concat_axis=0, tiled=True
    )
    gate_grads = returned_value.reshape(places)[second_places]
    grad_scaled = gate_column * grad_hidden
    grad_gate = grad_scaled * up_part * squash * (1.0 + gate_part * (1.0 - squash))
    grad_up = grad_scaled * swish
    grad_both = jnp.concatenate([grad_gate, grad_up], axis=1).astype(jnp.bfloat16)
    grad_rows = (gate_column * incoming.astype(jnp.float32)).astype(jnp.bfloat16)
    down_term = lax.dot_general(
        activated_b, grad_rows, (((0,), (0,)), ((), ())), preferred_element_type=jnp.float32
    )
    gate_up_term = lax.dot_general(
        saved_rows, grad_both, (((0,), (0,)), ((), ())), preferred_element_type=jnp.float32
    )
    gate_up_grad, down_grad = (
        lax.psum_scatter(
            gate_up_term[None].astype(jnp.bfloat16), "dp", scatter_dimension=1, tiled=True
        ).astype(jnp.float32),
        lax.psum_scatter(
            down_term[None].astype(jnp.bfloat16), "dp", scatter_dimension=2, tiled=True
        ).astype(jnp.float32),
    )
    return (
        mixed_first,
        gate_grads,
        gate_up_grad.astype(jnp.bfloat16),
        down_grad.astype(jnp.bfloat16),
    )


MESH = pl.DeviceIdType.MESH
F32 = jnp.float32
BF16 = jnp.bfloat16


def flipped(index, offset):
    result, bit = index, 1
    while bit <= offset:
        if offset & bit:
            result = result + bit * (1 - 2 * ((index // bit) % 2))
        bit *= 2
    return result


def kernel(
    n_ep,
    n_dp,
    cap,
    routes_1_hbm,
    gates_1_hbm,
    routes_2_hbm,
    gates_2_hbm,
    tokens_hbm,
    upstream_hbm,
    gu_hbm,
    down_hbm,
    saved_hbm,
    rets,
    lookup,
    ggrad_ref,
    gu_out,
    dn_out,
    routes_1,
    gates_1,
    routes_2,
    gates_2,
    tokens,
    upstream,
    gu,
    down,
    saved,
    send_1,
    send_2,
    recv_1,
    recv_2,
    outs,
    proj,
    act_b,
    both,
    val_send,
    val_recv,
    term_gu,
    term_dn,
    pair_gu,
    pair_dn,
    sum_gu,
    sum_dn,
    far_gu,
    far_dn,
    in_sem,
    d2_send,
    d2_recv,
    d1_send,
    d1_recv,
    r1_send,
    r1_recv,
    v_send,
    v_recv,
    p_send,
    p_recv,
    f_send,
    f_recv,
):
    me = lax.axis_index("ep")
    me_dp = lax.axis_index("dp")
    parity, chip = me_dp % 2, me_dp // 2
    half = n_dp // 2
    mate = me_dp + 1 - 2 * parity
    count, width = tokens.shape
    hidden = down.shape[0]
    places = n_ep * cap
    middle = n_ep // 2
    near = list(range(middle - 1, 0, -1))
    cross = list(range(middle, n_ep))
    order = near + cross

    quarter = me // (n_ep // 4)
    inner = (quarter == 1) | (quarter == 2)
    outer = (quarter == 0) | (quarter == 3)

    loads = [
        pltpu.make_async_copy(source, target, in_sem.at[k])
        for k, (source, target) in enumerate(
            (
                (routes_2_hbm, routes_2),
                (gates_2_hbm, gates_2),
                (upstream_hbm, upstream),
                (routes_1_hbm, routes_1),
                (gates_1_hbm, gates_1),
                (tokens_hbm, tokens),
                (saved_hbm, saved),
                (gu_hbm, gu),
                (down_hbm, down),
            )
        )
    ]
    for copy in loads[:3]:
        copy.start()

    barrier = pltpu.get_barrier_semaphore()
    for d in range(n_ep - 1, 0, -1):
        pl.semaphore_signal(
            barrier, inc=1, device_id=(flipped(me, d), me_dp), device_id_type=MESH
        )
    pl.semaphore_signal(barrier, inc=1, device_id=(me, mate), device_id_type=MESH)
    for t in range(1, half):
        pl.semaphore_signal(
            barrier,
            inc=1,
            device_id=(me, 2 * ((chip + t) % half) + parity),
            device_id_type=MESH,
        )

    def remote(source, target, sends, recvs, to):
        return pltpu.make_async_remote_copy(
            src_ref=source,
            dst_ref=target,
            send_sem=sends,
            recv_sem=recvs,
            device_id=to,
            device_id_type=MESH,
        )

    def placed(routes_ref):
        routes = routes_ref[...]
        rank = lax.broadcasted_iota(jnp.int32, (max(n_ep, 16), count), 0)
        named = jnp.where(rank == routes, 1.0, 0.0)
        earlier = jnp.where(
            lax.broadcasted_iota(jnp.int32, (count, count), 0)
            < lax.broadcasted_iota(jnp.int32, (count, count), 1),
            1.0,
            0.0,
        ).astype(BF16)
        before = jnp.dot(named.astype(BF16), earlier, preferred_element_type=F32)
        slots = jnp.sum(named * before, axis=0, keepdims=True).astype(jnp.int32)
        offset = jnp.bitwise_xor(routes, me)
        return offset, slots

    def column(row):
        return jnp.broadcast_to(row.astype(F32), (count, count)).T

    def spread(select, values, target, low, high):
        target[low:high] = (
            jnp.dot(select[low * cap : high * cap], values[...], preferred_element_type=F32)
            .astype(BF16)
            .reshape(high - low, cap, width)
        )

    slot_ids = lax.broadcasted_iota(jnp.int32, (places, count), 0)

    def turned(d):
        if d == 1:
            return d, flipped(me, 1)
        base = flipped(me, d - d % 2)
        swap = parity + (d % 2) * (1 - 2 * parity)
        return d - d % 2 + swap, base + swap * (1 - 2 * (base % 2))

    def start(kind, numbers):
        source, target, sends, recvs = {
            1: (send_1, recv_1, d1_send, d1_recv),
            2: (send_2, recv_2, d2_send, d2_recv),
            3: (outs, rets, r1_send, r1_recv),
        }[kind]
        pieces = 2
        for pair in dict.fromkeys(d // 2 for d in numbers):
            for piece in range(pieces):
                rows = slice(piece * cap // pieces, (piece + 1) * cap // pieces)
                for number in numbers:
                    if number // 2 == pair:
                        d, to = turned(number)
                        remote(
                            source.at[d, rows],
                            target.at[me if kind == 2 else d, rows],
                            sends,
                            recvs.at[pair] if kind == 1 else recvs,
                            (to, me_dp),
                        ).start()

    def several(source, target, sends, recvs):
        return remote(source, target, sends, recvs, (me, mate))


    loads[0].wait()
    offset_2, slot_2 = placed(routes_2)
    place_2 = offset_2 * cap + slot_2
    loads[1].wait()
    gate_row_2 = gates_2[...].astype(F32)
    select_2 = jnp.where(slot_ids == place_2, gate_row_2, 0.0).astype(BF16)
    loads[2].wait()
    for copy in loads[3:]:
        copy.start()
    spread(select_2, upstream, send_2, middle, n_ep)
    pl.semaphore_wait(barrier, n_ep - 1 + half)

    @pl.when(inner)
    def _():
        start(2, cross[middle // 2 :] + cross[: middle // 2])

    spread(select_2, upstream, send_2, 0, middle)
    start(2, near)

    @pl.when(outer)
    def _():
        start(2, cross)

    recv_2[me] = send_2[0]

    loads[3].wait()
    loads[4].wait()
    offset_1, slot_1 = placed(routes_1)
    place_1 = offset_1 * cap + slot_1
    select_1 = jnp.where(slot_ids == place_1, 1.0, 0.0).astype(BF16)
    loads[5].wait()
    spread(select_1, tokens, send_1, 0, n_ep)
    recv_1[0] = send_1[0]

    start(1, near)

    @pl.when(inner)
    def _():
        start(1, cross)


    place_col = column(place_1)
    gate_col = column(gates_1[...])
    lane_col = lax.broadcasted_iota(jnp.int32, (count, 128), 1).astype(F32)
    for part in range(places // 128):
        lookup[:, part * 128 : (part + 1) * 128] = jnp.where(
            place_col[:, :128] == lane_col + float(128 * part), gate_col[:, :128], 0.0
        ).astype(BF16)

    loads[6].wait()
    loads[7].wait()
    proj[...] = jnp.dot(saved[...], gu[...], preferred_element_type=F32)
    gate = proj[:, :hidden]
    act_b[...] = (gate * jax.nn.sigmoid(gate) * proj[:, hidden:]).astype(BF16)
    loads[8].wait()

    others = slice(1, n_ep)
    several(send_2.at[others], recv_2.at[others], d2_send, d2_recv).wait_recv()

    @pl.when(outer)
    def _():
        start(1, cross)


    incoming = recv_2[...].reshape(places, width)
    scaled = lax.dot_general(
        incoming, down[...], (((1,), (1,)), ((), ())), preferred_element_type=F32
    )
    product = scaled * act_b[...].astype(F32)
    lanes = product[:, :128]
    for first in range(128, hidden, 128):
        lanes = lanes + product[:, first : first + 128]
    values = jnp.sum(lanes.T, axis=0, keepdims=True)
    val_send[...] = values
    val_recv[0] = values
    move_v = {}
    for d in order:
        move_v[d] = remote(
            val_send, val_recv.at[d], v_send, v_recv, (flipped(me, d), me_dp)
        )
        move_v[d].start()
    gate = proj[:, :hidden]
    squash = jax.nn.sigmoid(gate)
    both[:, :hidden] = (
        scaled * proj[:, hidden:] * squash * (1.0 + gate * (1.0 - squash))
    ).astype(BF16)
    both[:, hidden:] = (scaled * (gate * squash)).astype(BF16)

    rows_gu = width // n_dp
    activated_b = act_b[...]
    for j in range(n_dp):
        term_gu[j] = lax.dot_general(
            saved[:, j * rows_gu : (j + 1) * rows_gu],
            both[...],
            (((0,), (0,)), ((), ())),
            preferred_element_type=F32,
        ).astype(BF16)
        term_dn[j] = lax.dot_general(
            activated_b,
            incoming[:, j * rows_gu : (j + 1) * rows_gu],
            (((0,), (0,)), ((), ())),
            preferred_element_type=F32,
        ).astype(BF16)
    for k in range(half):
        for kind, (term, pair) in enumerate(((term_gu, pair_gu), (term_dn, pair_dn))):
            remote(
                term.at[2 * k + 1 - parity],
                pair.at[k],
                p_send.at[kind],
                p_recv.at[kind],
                (me, mate),
            ).start()
    moved_p = [
        several(term.at[:half], pair, p_send.at[kind], p_recv.at[kind])
        for kind, (term, pair) in enumerate(((term_gu, pair_gu), (term_dn, pair_dn)))
    ]
    for copy in moved_p:
        copy.wait_recv()
    for t in range(1, half):
        k = (chip + t) % half
        for kind, (term, pair, joint, far) in enumerate(
            ((term_gu, pair_gu, sum_gu, far_gu), (term_dn, pair_dn, sum_dn, far_dn))
        ):
            joint[t - 1] = (
                term[2 * k + parity].astype(F32) + pair[k].astype(F32)
            ).astype(BF16)
            remote(
                joint.at[t - 1],
                far.at[t - 1],
                f_send.at[kind],
                f_recv.at[kind],
                (me, 2 * k + parity),
            ).start()
    moved_f = [
        several(joint, far, f_send.at[kind], f_recv.at[kind])
        for kind, (joint, far) in enumerate(((sum_gu, far_gu), (sum_dn, far_dn)))
    ]

    groups = list(range(n_ep // 4 - 1, -1, -1)) + list(range(n_ep // 4, n_ep // 2))
    for g in groups:
        pair = slice(2 * g if g else 1, 2 * g + 2)
        several(send_1.at[pair], recv_1.at[pair], d1_send, d1_recv.at[g]).wait_recv()
        rows = recv_1[2 * g : 2 * g + 2].reshape(2 * cap, width)
        projected = jnp.dot(rows, gu[...], preferred_element_type=F32)
        first_gate = projected[:, :hidden]
        activated = (first_gate * jax.nn.sigmoid(first_gate) * projected[:, hidden:]).astype(BF16)
        outs[2 * g : 2 * g + 2] = (
            jnp.dot(activated, down[...], preferred_element_type=F32)
            .astype(BF16)
            .reshape(2, cap, width)
        )
        start(3, [d for d in (2 * g, 2 * g + 1) if d])
        if g == 0:
            rets[0] = outs[0]

    several(val_recv.at[others], val_recv.at[others], v_send, v_recv).wait_recv()
    offset_col = column(offset_2)
    wanted = column(slot_2 + me * cap)
    lane_ids = lax.broadcasted_iota(jnp.int32, (count, 128), 1).astype(F32)
    picked = jnp.zeros((count, 128), F32)
    for part in range(places // 128):
        for d in range(n_ep):
            hit = (offset_col[:, :128] == float(d)) & (wanted[:, :128] == lane_ids + 128.0 * part)
            picked = picked + jnp.where(hit, val_recv[d, :, part * 128 : (part + 1) * 128], 0.0)
    ggrad_ref[...] = jnp.sum(picked.T, axis=0, keepdims=True) / gate_row_2

    for copy in moved_f:
        copy.wait_recv()
    for term, pair, far, out in (
        (term_gu, pair_gu, far_gu, gu_out),
        (term_dn, pair_dn, far_dn, dn_out),
    ):
        result = term[me_dp].astype(F32) + pair[chip].astype(F32)
        for t in range(1, half):
            result = result + far[t - 1].astype(F32)
        out[...] = result.astype(BF16)

    several(send_2.at[others], recv_2.at[others], d2_send, d2_recv).wait_send()
    several(send_1.at[others], recv_1.at[others], d1_send, d1_recv.at[0]).wait_send()
    several(val_recv.at[others], val_recv.at[others], v_send, v_recv).wait_send()
    for copy in moved_p + moved_f:
        copy.wait_send()
    returned = several(outs.at[others], rets.at[others], r1_send, r1_recv)
    returned.wait_send()
    returned.wait_recv()


def finish(
    rets, lookup, ggrad, gu_grad, dn_grad, mixed_hbm, ggrad_hbm, gu_hbm, dn_hbm, mixed, out_sem
):
    stores = [
        pltpu.make_async_copy(source, target, out_sem.at[k])
        for k, (source, target) in enumerate(
            ((gu_grad, gu_hbm), (dn_grad, dn_hbm), (ggrad, ggrad_hbm))
        )
    ]
    for copy in stores:
        copy.start()
    width = mixed.shape[1]
    slots = rets.shape[0] * rets.shape[1]
    step = width // 4
    for number in range(4):
        columns = slice(number * step, (number + 1) * step)
        mixed[:, columns] = jnp.dot(
            lookup[...], rets[:, :, columns].reshape(slots, step), preferred_element_type=F32
        ).astype(BF16)
        copy = pltpu.make_async_copy(
            mixed.at[:, columns], mixed_hbm.at[:, columns], out_sem.at[3 + number]
        )
        copy.start()
        stores.append(copy)
    for copy in stores:
        copy.wait()


def local(
    tokens_first,
    routes_first,
    gates_first,
    gate_up_weight,
    down_weight,
    saved_inputs,
    upstream,
    routes_second,
    gates_second,
):
    n_ep, n_dp = lax.axis_size("ep"), lax.axis_size("dp")
    cap = saved_inputs.shape[2] // n_ep
    count, top = routes_first.shape
    width = tokens_first.shape[1]
    hidden = down_weight.shape[1]
    places = n_ep * cap
    fits = (
        top == 1
        and cap % 16 == 0
        and 2 * cap <= 128
        and count == 128
        and places % 128 == 0
        and hidden % 128 == 0
        and n_ep >= 4
        and n_ep & (n_ep - 1) == 0
        and n_dp >= 4
        and n_dp % 2 == 0
        and (width // n_dp) % 128 == 0
    )
    if not fits:
        return local_plain(
            tokens_first,
            routes_first,
            gates_first,
            gate_up_weight,
            down_weight,
            saved_inputs,
            upstream,
            routes_second,
            gates_second,
        )
    half, part = n_dp // 2, width // n_dp
    slots = pltpu.VMEM((n_ep, cap, width), BF16)
    dma = pltpu.SemaphoreType.DMA
    vmem, anywhere = pl.BlockSpec(memory_space=pltpu.VMEM), pl.BlockSpec(memory_space=pl.ANY)
    reached = pl.pallas_call(
        functools.partial(kernel, n_ep, n_dp, cap),
        out_shape=(
            slots,
            pltpu.VMEM((count, places), BF16),
            pltpu.VMEM((1, count), F32),
            pltpu.VMEM((part, 2 * hidden), BF16),
            pltpu.VMEM((hidden, part), BF16),
        ),
        in_specs=[anywhere] * 9,
        out_specs=(vmem,) * 5,
        scratch_shapes=[
            pltpu.VMEM((1, count), jnp.int32),
            pltpu.VMEM((1, count), BF16),
            pltpu.VMEM((1, count), jnp.int32),
            pltpu.VMEM((1, count), BF16),
            pltpu.VMEM((count, width), BF16),
            pltpu.VMEM((count, width), BF16),
            pltpu.VMEM((width, 2 * hidden), BF16),
            pltpu.VMEM((hidden, width), BF16),
            pltpu.VMEM((places, width), BF16),
            slots,
            slots,
            slots,
            slots,
            slots,
            pltpu.VMEM((places, 2 * hidden), F32),
            pltpu.VMEM((places, hidden), BF16),
            pltpu.VMEM((places, 2 * hidden), BF16),
            pltpu.VMEM((1, places), F32),
            pltpu.VMEM((n_ep, 1, places), F32),
            pltpu.VMEM((n_dp, part, 2 * hidden), BF16),
            pltpu.VMEM((n_dp, hidden, part), BF16),
            pltpu.VMEM((half, part, 2 * hidden), BF16),
            pltpu.VMEM((half, hidden, part), BF16),
            pltpu.VMEM((half - 1, part, 2 * hidden), BF16),
            pltpu.VMEM((half - 1, hidden, part), BF16),
            pltpu.VMEM((half - 1, part, 2 * hidden), BF16),
            pltpu.VMEM((half - 1, hidden, part), BF16),
            dma((9,)),
        ]
        + [dma(()), dma(()), dma(()), dma((n_ep // 2,))]
        + [dma(())] * 4
        + [dma((2,))] * 4,
        compiler_params=pltpu.CompilerParams(
            collective_id=0, has_side_effects=True, vmem_limit_bytes=44 * 1024 * 1024
        ),
    )(
        *(
            pltpu.with_memory_space_constraint(value, pltpu.HBM)
            for value in (
                routes_first.reshape(1, count),
                gates_first.reshape(1, count),
                routes_second.reshape(1, count),
                gates_second.reshape(1, count),
                tokens_first,
                upstream,
                gate_up_weight[0],
                down_weight[0],
                saved_inputs[0, 0],
            )
        )
    )
    mixed, gate_grads, gu_grad, dn_grad = pl.pallas_call(
        finish,
        out_shape=(
            jax.ShapeDtypeStruct((count, width), BF16),
            jax.ShapeDtypeStruct((1, count), F32),
            jax.ShapeDtypeStruct((part, 2 * hidden), BF16),
            jax.ShapeDtypeStruct((hidden, part), BF16),
        ),
        in_specs=[vmem] * 5,
        out_specs=(anywhere,) * 4,
        scratch_shapes=[pltpu.VMEM((count, width), BF16), dma((7,))],
        name="finish",
    )(*(pltpu.with_memory_space_constraint(value, pltpu.VMEM) for value in reached))
    return mixed, gate_grads.reshape(count, 1), gu_grad[None], dn_grad[None]


def solution(mesh):
    return jax.shard_map(
        local,
        mesh=mesh,
        in_specs=(
            P(("ep", "dp"), None),
            P(("ep", "dp"), None),
            P(("ep", "dp"), None),
            P("ep", None, None),
            P("ep", None, None),
            P("ep", "dp", None, None),
            P(("ep", "dp"), None),
            P(("ep", "dp"), None),
            P(("ep", "dp"), None),
        ),
        out_specs=(
            P(("ep", "dp"), None),
            P(("ep", "dp"), None),
            P("ep", "dp", None),
            P("ep", None, "dp"),
        ),
        check_vma=False,
    )
```

```python
import functools

import jax
import jax.numpy as jnp
from jax import lax
from jax.experimental import pallas as pl
from jax.experimental.pallas import tpu as pltpu
from jax.sharding import PartitionSpec as P


def slot_places(routing, experts, capacity):
    expert_ids = jnp.arange(experts, dtype=jnp.int32)
    onehot = (routing[:, :, None] == expert_ids).astype(jnp.int32)
    counts = jnp.sum(onehot, axis=1)
    before = jnp.cumsum(counts, axis=0) - counts
    slots = jnp.sum(onehot * before[:, None, :], axis=2)
    return routing * capacity + slots


def local_plain(
    tokens_first,
    routes_first,
    gates_first,
    gate_up_weight,
    down_weight,
    saved_inputs,
    upstream,
    routes_second,
    gates_second,
):
    experts = lax.axis_size("ep")
    capacity = saved_inputs.shape[2] // experts
    places = experts * capacity
    model_width = tokens_first.shape[1]
    weight_gu = gate_up_weight[0]
    weight_down = down_weight[0]
    hidden_size = weight_down.shape[0]

    def expand(places_of):
        lookup = (places_of[:, :, None] == jnp.arange(places, dtype=jnp.int32)).astype(jnp.bfloat16)
        return (lookup, jnp.sum(lookup, axis=1))

    def dispatch(select, values):
        moved = lax.dot_general(
            select, values, (((0,), (0,)), ((), ())), preferred_element_type=jnp.float32
        )
        return moved.astype(jnp.bfloat16).reshape(experts, capacity, model_width)

    def project(inputs):
        return jnp.dot(inputs, weight_gu, preferred_element_type=jnp.float32)

    first_places = slot_places(routes_first, experts, capacity)
    first_lookup, first_select = expand(first_places)
    send_first = dispatch(first_select, tokens_first)
    second_places = slot_places(routes_second, experts, capacity)
    second_lookup, second_select = expand(second_places)
    send_grad = dispatch(second_select, upstream)
    send_gates = jnp.einsum(
        "tkp,tk->p",
        second_lookup.astype(jnp.float32),
        gates_second.astype(jnp.float32),
        precision=lax.Precision.HIGHEST,
    )
    send_gates = send_gates.astype(jnp.bfloat16).reshape(experts, capacity)
    received = lax.all_to_all(send_first, "ep", split_axis=0, concat_axis=0, tiled=True)
    sources = received.shape[0]
    items = received.shape[1]
    projected = project(received.reshape(sources * items, model_width))
    activated = (jax.nn.silu(projected[:, :hidden_size]) * projected[:, hidden_size:]).astype(
        jnp.bfloat16
    )
    outputs = jnp.dot(activated, weight_down, preferred_element_type=jnp.float32).astype(
        jnp.bfloat16
    )
    returned = lax.all_to_all(
        outputs.reshape(sources, items, model_width), "ep", split_axis=0, concat_axis=0, tiled=True
    )
    arrived_grad, arrived_gates = (
        lax.all_to_all(send_grad, "ep", split_axis=0, concat_axis=0, tiled=True),
        lax.all_to_all(send_gates, "ep", split_axis=0, concat_axis=0, tiled=True),
    )
    picked = returned.reshape(places, model_width)[first_places]
    mixed_first = jnp.sum(
        gates_first.astype(jnp.float32)[:, :, None] * picked.astype(jnp.float32), axis=1
    ).astype(jnp.bfloat16)
    saved_rows = saved_inputs[0, 0]
    projected_b = project(saved_rows)
    gate_part = projected_b[:, :hidden_size]
    up_part = projected_b[:, hidden_size:]
    squash = jax.nn.sigmoid(gate_part)
    swish = jax.nn.silu(gate_part)
    activated_b = (swish * up_part).astype(jnp.bfloat16)
    incoming = arrived_grad.reshape(places, model_width)
    gate_column = arrived_gates.reshape(places, 1).astype(jnp.float32)
    grad_hidden = lax.dot_general(
        incoming, weight_down, (((1,), (1,)), ((), ())), preferred_element_type=jnp.float32
    )
    slot_value = jnp.sum(grad_hidden * activated_b.astype(jnp.float32), axis=1)
    returned_value = lax.all_to_all(
        slot_value.reshape(experts, capacity), "ep", split_axis=0, concat_axis=0, tiled=True
    )
    gate_grads = returned_value.reshape(places)[second_places]
    grad_scaled = gate_column * grad_hidden
    grad_gate = grad_scaled * up_part * squash * (1.0 + gate_part * (1.0 - squash))
    grad_up = grad_scaled * swish
    grad_both = jnp.concatenate([grad_gate, grad_up], axis=1).astype(jnp.bfloat16)
    grad_rows = (gate_column * incoming.astype(jnp.float32)).astype(jnp.bfloat16)
    down_term = lax.dot_general(
        activated_b, grad_rows, (((0,), (0,)), ((), ())), preferred_element_type=jnp.float32
    )
    gate_up_term = lax.dot_general(
        saved_rows, grad_both, (((0,), (0,)), ((), ())), preferred_element_type=jnp.float32
    )
    gate_up_grad, down_grad = (
        lax.psum_scatter(
            gate_up_term[None].astype(jnp.bfloat16), "dp", scatter_dimension=1, tiled=True
        ).astype(jnp.float32),
        lax.psum_scatter(
            down_term[None].astype(jnp.bfloat16), "dp", scatter_dimension=2, tiled=True
        ).astype(jnp.float32),
    )
    return (
        mixed_first,
        gate_grads,
        gate_up_grad.astype(jnp.bfloat16),
        down_grad.astype(jnp.bfloat16),
    )


MESH = pl.DeviceIdType.MESH
F32 = jnp.float32
BF16 = jnp.bfloat16


def flipped(index, offset):
    result, bit = index, 1
    while bit <= offset:
        if offset & bit:
            result = result + bit * (1 - 2 * ((index // bit) % 2))
        bit *= 2
    return result


def kernel(
    n_ep,
    n_dp,
    cap,
    routes_1_hbm,
    gates_1_hbm,
    routes_2_hbm,
    gates_2_hbm,
    tokens_hbm,
    upstream_hbm,
    gu_hbm,
    down_hbm,
    saved_hbm,
    rets,
    lookup,
    ggrad_ref,
    gu_out,
    dn_out,
    routes_1,
    gates_1,
    routes_2,
    gates_2,
    tokens,
    upstream,
    gu,
    down,
    saved,
    send_1,
    send_2,
    recv_1,
    recv_2,
    outs,
    proj,
    act_b,
    both,
    val_send,
    val_recv,
    term_gu,
    term_dn,
    pair_gu,
    pair_dn,
    sum_gu,
    sum_dn,
    far_gu,
    far_dn,
    in_sem,
    d2_send,
    d2_recv,
    d1_send,
    d1_recv,
    r1_send,
    r1_recv,
    v_send,
    v_recv,
    p_send,
    p_recv,
    f_send,
    f_recv,
):
    me = lax.axis_index("ep")
    me_dp = lax.axis_index("dp")
    parity, chip = me_dp % 2, me_dp // 2
    half = n_dp // 2
    mate = me_dp + 1 - 2 * parity
    count, width = tokens.shape
    hidden = down.shape[0]
    places = n_ep * cap
    middle = n_ep // 2
    near = list(range(middle - 1, 0, -1))
    cross = list(range(middle, n_ep))
    order = near + cross

    quarter = me // (n_ep // 4)
    inner = (quarter == 1) | (quarter == 2)
    outer = (quarter == 0) | (quarter == 3)

    loads = [
        pltpu.make_async_copy(source, target, in_sem.at[k])
        for k, (source, target) in enumerate(
            (
                (routes_2_hbm, routes_2),
                (gates_2_hbm, gates_2),
                (upstream_hbm, upstream),
                (routes_1_hbm, routes_1),
                (gates_1_hbm, gates_1),
                (tokens_hbm, tokens),
                (saved_hbm, saved),
                (gu_hbm, gu),
                (down_hbm, down),
            )
        )
    ]
    for copy in loads[:3]:
        copy.start()

    kin = [d for d in range(n_ep - 1, 0, -1) if d // (n_ep // 4) in (0, 3)]
    strange = [d for d in range(n_ep - 1, 0, -1) if d not in kin]
    barrier = pltpu.get_barrier_semaphore()

    def greet(numbers):
        for d in numbers:
            pl.semaphore_signal(
                barrier, inc=1, device_id=(flipped(me, d), me_dp), device_id_type=MESH
            )

    greet(kin)
    pl.semaphore_signal(barrier, inc=1, device_id=(me, mate), device_id_type=MESH)
    for t in range(1, half):
        pl.semaphore_signal(
            barrier,
            inc=1,
            device_id=(me, 2 * ((chip + t) % half) + parity),
            device_id_type=MESH,
        )

    def remote(source, target, sends, recvs, to):
        return pltpu.make_async_remote_copy(
            src_ref=source,
            dst_ref=target,
            send_sem=sends,
            recv_sem=recvs,
            device_id=to,
            device_id_type=MESH,
        )

    def placed(routes_ref):
        routes = routes_ref[...]
        rank = lax.broadcasted_iota(jnp.int32, (max(n_ep, 16), count), 0)
        named = jnp.where(rank == routes, 1.0, 0.0)
        earlier = jnp.where(
            lax.broadcasted_iota(jnp.int32, (count, count), 0)
            < lax.broadcasted_iota(jnp.int32, (count, count), 1),
            1.0,
            0.0,
        ).astype(BF16)
        before = jnp.dot(named.astype(BF16), earlier, preferred_element_type=F32)
        slots = jnp.sum(named * before, axis=0, keepdims=True).astype(jnp.int32)
        offset = jnp.bitwise_xor(routes, me)
        return offset, slots

    def column(row):
        return jnp.broadcast_to(row.astype(F32), (count, count)).T

    def spread(select, values, target, low, high):
        target[low:high] = (
            jnp.dot(select[low * cap : high * cap], values[...], preferred_element_type=F32)
            .astype(BF16)
            .reshape(high - low, cap, width)
        )

    slot_ids = lax.broadcasted_iota(jnp.int32, (places, count), 0)

    def turned(d, side):
        if d == 1:
            return d, flipped(me, 1)
        base = flipped(me, d - d % 2)
        swap = side + (d % 2) * (1 - 2 * side)
        return d - d % 2 + swap, base + swap * (1 - 2 * (base % 2))

    def start(kind, numbers):
        source, target, sends, recvs = {
            1: (send_1, recv_1, d1_send, d1_recv),
            2: (send_2, recv_2, d2_send, d2_recv),
            3: (outs, rets, r1_send, r1_recv),
        }[kind]
        pieces = 2
        for pair in dict.fromkeys(d // 2 for d in numbers):
            members = [d for d in numbers if d // 2 == pair]
            last = kind == 3 and pair == n_ep // 2 - 1
            pairs = [(piece, number) for piece in range(pieces) for number in members]
            if last:
                pairs.sort(key=lambda entry: entry[1])
            for piece, number in pairs:
                rows = slice(piece * cap // pieces, (piece + 1) * cap // pieces)
                d, to = turned(number, me % 2 if last else parity)
                remote(
                    source.at[d, rows],
                    target.at[me if kind == 2 else d, rows],
                    sends,
                    recvs.at[pair] if kind == 1 else recvs,
                    (to, me_dp),
                ).start()

    def several(source, target, sends, recvs):
        return remote(source, target, sends, recvs, (me, mate))


    loads[0].wait()
    offset_2, slot_2 = placed(routes_2)
    place_2 = offset_2 * cap + slot_2
    loads[1].wait()
    gate_row_2 = gates_2[...].astype(F32)
    select_2 = jnp.where(slot_ids == place_2, gate_row_2, 0.0).astype(BF16)
    loads[2].wait()
    for copy in loads[3:]:
        copy.start()
    spread(select_2, upstream, send_2, middle, n_ep)
    ahead, behind = cross[middle // 2 :], cross[: middle // 2]

    @pl.when(inner)
    def _():
        pl.semaphore_wait(barrier, len(kin) + half)
        greet(strange)
        start(2, ahead)

    spread(select_2, upstream, send_2, 0, middle)
    recv_2[me] = send_2[0]

    @pl.when(outer)
    def _():
        pl.semaphore_wait(barrier, len(kin) + half + len(strange))
        greet(strange)
        start(2, order)

    loads[3].wait()
    loads[4].wait()
    offset_1, slot_1 = placed(routes_1)
    place_1 = offset_1 * cap + slot_1
    select_1 = jnp.where(slot_ids == place_1, 1.0, 0.0).astype(BF16)
    loads[5].wait()
    spread(select_1, tokens, send_1, 0, n_ep)
    recv_1[0] = send_1[0]

    @pl.when(inner)
    def _():
        pl.semaphore_wait(barrier, len(strange))
        start(2, near + behind)
        start(1, near + cross)

    @pl.when(outer)
    def _():
        start(1, near)

    place_col = column(place_1)
    gate_col = column(gates_1[...])
    lane_col = lax.broadcasted_iota(jnp.int32, (count, 128), 1).astype(F32)
    for part in range(places // 128):
        lookup[:, part * 128 : (part + 1) * 128] = jnp.where(
            place_col[:, :128] == lane_col + float(128 * part), gate_col[:, :128], 0.0
        ).astype(BF16)

    loads[6].wait()
    loads[7].wait()
    proj[...] = jnp.dot(saved[...], gu[...], preferred_element_type=F32)
    gate = proj[:, :hidden]
    act_b[...] = (gate * jax.nn.sigmoid(gate) * proj[:, hidden:]).astype(BF16)
    loads[8].wait()

    others = slice(1, n_ep)
    several(send_2.at[others], recv_2.at[others], d2_send, d2_recv).wait_recv()

    @pl.when(outer)
    def _():
        start(1, cross)


    incoming = recv_2[...].reshape(places, width)
    scaled = lax.dot_general(
        incoming, down[...], (((1,), (1,)), ((), ())), preferred_element_type=F32
    )
    product = scaled * act_b[...].astype(F32)
    lanes = product[:, :128]
    for first in range(128, hidden, 128):
        lanes = lanes + product[:, first : first + 128]
    values = jnp.sum(lanes.T, axis=0, keepdims=True)
    val_send[...] = values
    val_recv[0] = values
    move_v = {}
    for d in order:
        move_v[d] = remote(
            val_send, val_recv.at[d], v_send, v_recv, (flipped(me, d), me_dp)
        )
        move_v[d].start()
    gate = proj[:, :hidden]
    squash = jax.nn.sigmoid(gate)
    both[:, :hidden] = (
        scaled * proj[:, hidden:] * squash * (1.0 + gate * (1.0 - squash))
    ).astype(BF16)
    both[:, hidden:] = (scaled * (gate * squash)).astype(BF16)

    rows_gu = width // n_dp
    activated_b = act_b[...]
    for j in range(n_dp):
        term_gu[j] = lax.dot_general(
            saved[:, j * rows_gu : (j + 1) * rows_gu],
            both[...],
            (((0,), (0,)), ((), ())),
            preferred_element_type=F32,
        ).astype(BF16)
        term_dn[j] = lax.dot_general(
            activated_b,
            incoming[:, j * rows_gu : (j + 1) * rows_gu],
            (((0,), (0,)), ((), ())),
            preferred_element_type=F32,
        ).astype(BF16)
    for k in range(half):
        for kind, (term, pair) in enumerate(((term_gu, pair_gu), (term_dn, pair_dn))):
            remote(
                term.at[2 * k + 1 - parity],
                pair.at[k],
                p_send.at[kind],
                p_recv.at[kind],
                (me, mate),
            ).start()
    moved_p = [
        several(term.at[:half], pair, p_send.at[kind], p_recv.at[kind])
        for kind, (term, pair) in enumerate(((term_gu, pair_gu), (term_dn, pair_dn)))
    ]
    for copy in moved_p:
        copy.wait_recv()
    for t in range(1, half):
        k = (chip + t) % half
        for kind, (term, pair, joint, far) in enumerate(
            ((term_gu, pair_gu, sum_gu, far_gu), (term_dn, pair_dn, sum_dn, far_dn))
        ):
            joint[t - 1] = (
                term[2 * k + parity].astype(F32) + pair[k].astype(F32)
            ).astype(BF16)
            remote(
                joint.at[t - 1],
                far.at[t - 1],
                f_send.at[kind],
                f_recv.at[kind],
                (me, 2 * k + parity),
            ).start()
    moved_f = [
        several(joint, far, f_send.at[kind], f_recv.at[kind])
        for kind, (joint, far) in enumerate(((sum_gu, far_gu), (sum_dn, far_dn)))
    ]

    groups = list(range(n_ep // 4 - 1, -1, -1)) + list(range(n_ep // 4, n_ep // 2))
    for g in groups:
        pair = slice(2 * g if g else 1, 2 * g + 2)
        several(send_1.at[pair], recv_1.at[pair], d1_send, d1_recv.at[g]).wait_recv()
        rows = recv_1[2 * g : 2 * g + 2].reshape(2 * cap, width)
        projected = jnp.dot(rows, gu[...], preferred_element_type=F32)
        first_gate = projected[:, :hidden]
        activated = (first_gate * jax.nn.sigmoid(first_gate) * projected[:, hidden:]).astype(BF16)
        outs[2 * g : 2 * g + 2] = (
            jnp.dot(activated, down[...], preferred_element_type=F32)
            .astype(BF16)
            .reshape(2, cap, width)
        )
        start(3, [d for d in (2 * g, 2 * g + 1) if d])
        if g == 0:
            rets[0] = outs[0]

    several(val_recv.at[others], val_recv.at[others], v_send, v_recv).wait_recv()
    offset_col = column(offset_2)
    wanted = column(slot_2 + me * cap)
    lane_ids = lax.broadcasted_iota(jnp.int32, (count, 128), 1).astype(F32)
    picked = jnp.zeros((count, 128), F32)
    for part in range(places // 128):
        for d in range(n_ep):
            hit = (offset_col[:, :128] == float(d)) & (wanted[:, :128] == lane_ids + 128.0 * part)
            picked = picked + jnp.where(hit, val_recv[d, :, part * 128 : (part + 1) * 128], 0.0)
    ggrad_ref[...] = jnp.sum(picked.T, axis=0, keepdims=True) / gate_row_2

    for copy in moved_f:
        copy.wait_recv()
    for term, pair, far, out in (
        (term_gu, pair_gu, far_gu, gu_out),
        (term_dn, pair_dn, far_dn, dn_out),
    ):
        result = term[me_dp].astype(F32) + pair[chip].astype(F32)
        for t in range(1, half):
            result = result + far[t - 1].astype(F32)
        out[...] = result.astype(BF16)

    several(send_2.at[others], recv_2.at[others], d2_send, d2_recv).wait_send()
    several(send_1.at[others], recv_1.at[others], d1_send, d1_recv.at[0]).wait_send()
    several(val_recv.at[others], val_recv.at[others], v_send, v_recv).wait_send()
    for copy in moved_p + moved_f:
        copy.wait_send()
    returned = several(outs.at[others], rets.at[others], r1_send, r1_recv)
    returned.wait_send()
    returned.wait_recv()


def finish(
    rets, lookup, ggrad, gu_grad, dn_grad, mixed_hbm, ggrad_hbm, gu_hbm, dn_hbm, mixed, out_sem
):
    stores = [
        pltpu.make_async_copy(source, target, out_sem.at[k])
        for k, (source, target) in enumerate(
            ((gu_grad, gu_hbm), (dn_grad, dn_hbm), (ggrad, ggrad_hbm))
        )
    ]
    for copy in stores:
        copy.start()
    width = mixed.shape[1]
    slots = rets.shape[0] * rets.shape[1]
    step = width // 4
    for number in range(4):
        columns = slice(number * step, (number + 1) * step)
        mixed[:, columns] = jnp.dot(
            lookup[...], rets[:, :, columns].reshape(slots, step), preferred_element_type=F32
        ).astype(BF16)
        copy = pltpu.make_async_copy(
            mixed.at[:, columns], mixed_hbm.at[:, columns], out_sem.at[3 + number]
        )
        copy.start()
        stores.append(copy)
    for copy in stores:
        copy.wait()


def local(
    tokens_first,
    routes_first,
    gates_first,
    gate_up_weight,
    down_weight,
    saved_inputs,
    upstream,
    routes_second,
    gates_second,
):
    n_ep, n_dp = lax.axis_size("ep"), lax.axis_size("dp")
    cap = saved_inputs.shape[2] // n_ep
    count, top = routes_first.shape
    width = tokens_first.shape[1]
    hidden = down_weight.shape[1]
    places = n_ep * cap
    fits = (
        top == 1
        and cap % 16 == 0
        and 2 * cap <= 128
        and count == 128
        and places % 128 == 0
        and hidden % 128 == 0
        and n_ep >= 4
        and n_ep & (n_ep - 1) == 0
        and n_dp >= 4
        and n_dp % 2 == 0
        and (width // n_dp) % 128 == 0
    )
    if not fits:
        return local_plain(
            tokens_first,
            routes_first,
            gates_first,
            gate_up_weight,
            down_weight,
            saved_inputs,
            upstream,
            routes_second,
            gates_second,
        )
    half, part = n_dp // 2, width // n_dp
    slots = pltpu.VMEM((n_ep, cap, width), BF16)
    dma = pltpu.SemaphoreType.DMA
    vmem, anywhere = pl.BlockSpec(memory_space=pltpu.VMEM), pl.BlockSpec(memory_space=pl.ANY)
    reached = pl.pallas_call(
        functools.partial(kernel, n_ep, n_dp, cap),
        out_shape=(
            slots,
            pltpu.VMEM((count, places), BF16),
            pltpu.VMEM((1, count), F32),
            pltpu.VMEM((part, 2 * hidden), BF16),
            pltpu.VMEM((hidden, part), BF16),
        ),
        in_specs=[anywhere] * 9,
        out_specs=(vmem,) * 5,
        scratch_shapes=[
            pltpu.VMEM((1, count), jnp.int32),
            pltpu.VMEM((1, count), BF16),
            pltpu.VMEM((1, count), jnp.int32),
            pltpu.VMEM((1, count), BF16),
            pltpu.VMEM((count, width), BF16),
            pltpu.VMEM((count, width), BF16),
            pltpu.VMEM((width, 2 * hidden), BF16),
            pltpu.VMEM((hidden, width), BF16),
            pltpu.VMEM((places, width), BF16),
            slots,
            slots,
            slots,
            slots,
            slots,
            pltpu.VMEM((places, 2 * hidden), F32),
            pltpu.VMEM((places, hidden), BF16),
            pltpu.VMEM((places, 2 * hidden), BF16),
            pltpu.VMEM((1, places), F32),
            pltpu.VMEM((n_ep, 1, places), F32),
            pltpu.VMEM((n_dp, part, 2 * hidden), BF16),
            pltpu.VMEM((n_dp, hidden, part), BF16),
            pltpu.VMEM((half, part, 2 * hidden), BF16),
            pltpu.VMEM((half, hidden, part), BF16),
            pltpu.VMEM((half - 1, part, 2 * hidden), BF16),
            pltpu.VMEM((half - 1, hidden, part), BF16),
            pltpu.VMEM((half - 1, part, 2 * hidden), BF16),
            pltpu.VMEM((half - 1, hidden, part), BF16),
            dma((9,)),
        ]
        + [dma(()), dma(()), dma(()), dma((n_ep // 2,))]
        + [dma(())] * 4
        + [dma((2,))] * 4,
        compiler_params=pltpu.CompilerParams(
            collective_id=0, has_side_effects=True, vmem_limit_bytes=44 * 1024 * 1024
        ),
    )(
        *(
            pltpu.with_memory_space_constraint(value, pltpu.HBM)
            for value in (
                routes_first.reshape(1, count),
                gates_first.reshape(1, count),
                routes_second.reshape(1, count),
                gates_second.reshape(1, count),
                tokens_first,
                upstream,
                gate_up_weight[0],
                down_weight[0],
                saved_inputs[0, 0],
            )
        )
    )
    mixed, gate_grads, gu_grad, dn_grad = pl.pallas_call(
        finish,
        out_shape=(
            jax.ShapeDtypeStruct((count, width), BF16),
            jax.ShapeDtypeStruct((1, count), F32),
            jax.ShapeDtypeStruct((part, 2 * hidden), BF16),
            jax.ShapeDtypeStruct((hidden, part), BF16),
        ),
        in_specs=[vmem] * 5,
        out_specs=(anywhere,) * 4,
        scratch_shapes=[pltpu.VMEM((count, width), BF16), dma((7,))],
        name="finish",
    )(*(pltpu.with_memory_space_constraint(value, pltpu.VMEM) for value in reached))
    return mixed, gate_grads.reshape(count, 1), gu_grad[None], dn_grad[None]


def solution(mesh):
    return jax.shard_map(
        local,
        mesh=mesh,
        in_specs=(
            P(("ep", "dp"), None),
            P(("ep", "dp"), None),
            P(("ep", "dp"), None),
            P("ep", None, None),
            P("ep", None, None),
            P("ep", "dp", None, None),
            P(("ep", "dp"), None),
            P(("ep", "dp"), None),
            P(("ep", "dp"), None),
        ),
        out_specs=(
            P(("ep", "dp"), None),
            P(("ep", "dp"), None),
            P("ep", "dp", None),
            P("ep", None, "dp"),
        ),
        check_vma=False,
    )
```
